32 devices in a mesh: rep: 2 (over x), dp: 16 (over y, z, core).
Axes of the slice: x: 2, y: 2, z: 4, core: 2. Of those that a mesh axis runs over, the one named last changes fastest.
Arguments:
- x: bfloat16 [32, 2048, 512], P(('rep', 'dp')), parts along dimension 0
- dy: bfloat16 [32, 2048, 512], P(('rep', 'dp')), parts along dimension 0
- wq: bfloat16 [2, 512, 768], P(None, 'dp')
- wk: bfloat16 [2, 512, 128], P(None, 'dp')
- wv: bfloat16 [2, 512, 128], P(None, 'dp')
- wo: bfloat16 [2, 768, 512], P(None, 'dp')
- w_gate: bfloat16 [2, 512, 2048], P(None, 'dp')
- w_up: bfloat16 [2, 512, 2048], P(None, 'dp')
- w_down: bfloat16 [2, 2048, 512], P(None, 'dp')
- m_wq: float32 [2, 512, 768], P(None, 'dp')
- m_wk: float32 [2, 512, 128], P(None, 'dp')
- m_wv: float32 [2, 512, 128], P(None, 'dp')
- m_wo: float32 [2, 768, 512], P(None, 'dp')
- m_w_gate: float32 [2, 512, 2048], P(None, 'dp')
- m_w_up: float32 [2, 512, 2048], P(None, 'dp')
- m_w_down: float32 [2, 2048, 512], P(None, 'dp')
- v_wq: float32 [2, 512, 768], P(None, 'dp')
- v_wk: float32 [2, 512, 128], P(None, 'dp')
- v_wv: float32 [2, 512, 128], P(None, 'dp')
- v_wo: float32 [2, 768, 512], P(None, 'dp')
- v_w_gate: float32 [2, 512, 2048], P(None, 'dp')
- v_w_up: float32 [2, 512, 2048], P(None, 'dp')
- v_w_down: float32 [2, 2048, 512], P(None, 'dp')
Outputs:
- output 1: bfloat16 [4, 512, 768], P('rep', 'dp'), parts along dimension 0
- output 2: bfloat16 [4, 512, 128], P('rep', 'dp'), parts along dimension 0
- output 3: bfloat16 [4, 512, 128], P('rep', 'dp'), parts along dimension 0
- output 4: bfloat16 [4, 768, 512], P('rep', 'dp'), parts along dimension 0
- output 5: bfloat16 [4, 512, 2048], P('rep', 'dp'), parts along dimension 0
- output 6: bfloat16 [4, 512, 2048], P('rep', 'dp'), parts along dimension 0
- output 7: bfloat16 [4, 2048, 512], P('rep', 'dp'), parts along dimension 0
- output 8: float32 [4, 512, 768], P('rep', 'dp'), parts along dimension 0
- output 9: float32 [4, 512, 128], P('rep', 'dp'), parts along dimension 0
- output 10: float32 [4, 512, 128], P('rep', 'dp'), parts along dimension 0
- output 11: float32 [4, 768, 512], P('rep', 'dp'), parts along dimension 0
- output 12: float32 [4, 512, 2048], P('rep', 'dp'), parts along dimension 0
- output 13: float32 [4, 512, 2048], P('rep', 'dp'), parts along dimension 0
- output 14: float32 [4, 2048, 512], P('rep', 'dp'), parts along dimension 0
- output 15: float32 [4, 512, 768], P('rep', 'dp'), parts along dimension 0
- output 16: float32 [4, 512, 128], P('rep', 'dp'), parts along dimension 0
- output 17: float32 [4, 512, 128], P('rep', 'dp'), parts along dimension 0
- output 18: float32 [4, 768, 512], P('rep', 'dp'), parts along dimension 0
- output 19: float32 [4, 512, 2048], P('rep', 'dp'), parts along dimension 0
- output 20: float32 [4, 512, 2048], P('rep', 'dp'), parts along dimension 0
- output 21: float32 [4, 2048, 512], P('rep', 'dp'), parts along dimension 0
There are 2 independent parts. The reference program is written for one: setup_inputs(seed, part) draws one part's arguments, and reference() takes and returns one part's arrays. A program takes and returns all parts, laid end to end along the dimension named above; an argument that names none is the same for every part.
All inputs are finite; a program needn't handle non-finite values.
Results may differ from the reference program's by a relative error of at most 0.0248.
Values are sent between devices in bfloat16 or wider.
A program may use at most 2 GiB of HBM per device.

```python
import jax
import jax.numpy as jnp
from jax import lax

SEQUENCES = 16
TOKENS = 2048
D = 512
HEADS = 6
KV_HEADS = 1
HEAD = 128
FF = 2048
LAYERS = 2
THETA = 10000
NAMES = ("wq", "wk", "wv", "wo", "w_gate", "w_up", "w_down")
SHAPES = {
    "wq": (LAYERS, D, HEADS * HEAD),
    "wk": (LAYERS, D, KV_HEADS * HEAD),
    "wv": (LAYERS, D, KV_HEADS * HEAD),
    "wo": (LAYERS, HEADS * HEAD, D),
    "w_gate": (LAYERS, D, FF),
    "w_up": (LAYERS, D, FF),
    "w_down": (LAYERS, FF, D),
}


def bump(key, n, height):
    away = (jnp.arange(n, dtype=jnp.int32) - jax.random.randint(key, (), 0, n, jnp.int32)) % n
    return jnp.where(away < n // 8, height, 1.0)


def together(key, own, strength):
    shared = jax.random.normal(key, own.shape[1:], jnp.float32)
    return (own + strength * shared) * lax.rsqrt(1 + strength * strength)


def setup_inputs(seed: int = 0, part: int = 0) -> dict:
    kx, kdy, ka, kb, kz, kf, kh, kl, *keys = jax.random.split(jax.random.key(seed), 8 + 3 * len(NAMES))
    kx, kdy, ka, kb = (jax.random.fold_in(k, part) for k in (kx, kdy, ka, kb))
    kw, km, kv = (keys[i::3] for i in range(3))
    shape = (SEQUENCES, TOKENS, D)
    much_x, much_dy = jax.random.uniform(kz, (2,), jnp.float32, 0.0, 1.0)
    loud = 2.0 ** jax.random.uniform(jax.random.fold_in(kz, 1), (), jnp.float32, -1.0, 2.0)
    layers = 2.0 ** jax.random.uniform(kl, (LAYERS, 1, 1), jnp.float32, -1.0, 1.0)
    times = {"wq": 1.0, "wk": 1.0, "wv": 2.0, "wo": layers, "w_gate": 1.0, "w_up": bump(kh, FF, 4.0), "w_down": layers}
    x = together(ka, jax.random.normal(kx, shape, jnp.float32), much_x) * bump(kf, D, 4.0)
    dy = together(kb, jax.random.normal(kdy, shape, jnp.float32), much_dy)
    drawn = {"x": x.astype(jnp.bfloat16), "dy": (loud * dy * (SEQUENCES * TOKENS) ** -0.5).astype(jnp.bfloat16)}
    for key, name in zip(kw, NAMES, strict=True):
        drawn[name] = (jax.random.normal(key, SHAPES[name], jnp.float32) * SHAPES[name][1] ** -0.5 * times[name]).astype(jnp.bfloat16)
    for key, name in zip(km, NAMES, strict=True):
        drawn[f"m_{name}"] = 0.1 * jax.random.normal(key, SHAPES[name], jnp.float32)
    for key, name in zip(kv, NAMES, strict=True):
        drawn[f"v_{name}"] = jax.random.uniform(key, SHAPES[name], jnp.float32, 0.02, 0.06)
    return drawn


def matmul(a, w):
    return jnp.dot(a, w, preferred_element_type=jnp.float32).astype(jnp.bfloat16)


def normed(h):
    wide = h.astype(jnp.float32)
    scale = lax.rsqrt(jnp.mean(wide**2, -1, keepdims=True) + 1e-6)
    return (wide * scale).astype(jnp.bfloat16)


def turned(t, theta):
    half = t.shape[-1] // 2
    angle = jnp.arange(t.shape[0], dtype=jnp.float32)[:, None] * theta ** (-jnp.arange(half, dtype=jnp.float32) / half)
    cos, sin = jnp.cos(angle)[:, None], jnp.sin(angle)[:, None]
    a, b = t[..., :half].astype(jnp.float32), t[..., half:].astype(jnp.float32)
    return jnp.concatenate([a * cos - b * sin, b * cos + a * sin], -1).astype(jnp.bfloat16)


def seen_by(q, k, v):
    tokens, kv = q.shape[0], k.shape[1]
    q = q.reshape(tokens, kv, -1, q.shape[-1])
    scores = jnp.einsum("tgsd,ugd->gstu", q.astype(jnp.float32), k.astype(jnp.float32)) * q.shape[-1] ** -0.5
    place = jnp.arange(tokens)
    weights = jax.nn.softmax(jnp.where(place[:, None] >= place, scores, -jnp.inf), -1).astype(jnp.bfloat16)
    return jnp.einsum("gstu,ugd->tgsd", weights.astype(jnp.float32), v.astype(jnp.float32)).astype(jnp.bfloat16).reshape(tokens, -1)


def layer(h, w):
    a = normed(h)
    q, k = (turned(matmul(a, w[name]).reshape(h.shape[0], -1, HEAD), THETA) for name in ("wq", "wk"))
    h = h + matmul(seen_by(q, k, matmul(a, w["wv"]).reshape(h.shape[0], -1, HEAD)), w["wo"])
    b = normed(h)
    gate = jnp.dot(b, w["w_gate"], preferred_element_type=jnp.float32)
    up = jnp.dot(b, w["w_up"], preferred_element_type=jnp.float32)
    return h + matmul((jax.nn.silu(gate) * up).astype(jnp.bfloat16), w["w_down"])


def adamw(w, m, v, g):
    m = 0.9 * m + 0.1 * g
    v = 0.95 * v + 0.05 * g * g
    step = m * lax.rsqrt(v + 1e-8) + 0.1 * w
    return (w - 0.02 * step).astype(jnp.bfloat16), m, v


def clipped(gradients, sum_of_squares, count):
    factor = jnp.minimum(1.0, 0.5 * lax.rsqrt(sum_of_squares / count + 1e-30))
    return [g * factor for g in gradients]


def stack(weights, h):
    return lax.scan(lambda h, w: (layer(h, w), None), h, weights)[0]


def reference(x, dy, wq, wk, wv, wo, w_gate, w_up, w_down, m_wq, m_wk, m_wv, m_wo, m_w_gate, m_w_up, m_w_down, v_wq, v_wk, v_wv, v_wo, v_w_gate, v_w_up, v_w_down):
    weights = dict(zip(NAMES, (wq, wk, wv, wo, w_gate, w_up, w_down), strict=True))

    def take(so_far, sequence):
        h, by_y = sequence
        _, back = jax.vjp(stack, weights, h)
        by_weights, by_h = back(by_y)
        return jax.tree.map(lambda total, term: total + term.astype(jnp.float32), so_far, by_weights), by_h

    none_yet = {name: jnp.zeros(w.shape, jnp.float32) for name, w in weights.items()}
    by_weights, by_x = lax.scan(take, none_yet, (x, dy))
    gradients = [by_weights[name].astype(jnp.bfloat16).astype(jnp.float32) for name in NAMES]
    gradients = clipped(gradients, sum(jnp.sum(g * g) for g in gradients), sum(g.size for g in gradients))
    first = (m_wq, m_wk, m_wv, m_wo, m_w_gate, m_w_up, m_w_down)
    second = (v_wq, v_wk, v_wv, v_wo, v_w_gate, v_w_up, v_w_down)
    new = [adamw(weights[name].astype(jnp.float32), m, v, g) for name, m, v, g in zip(NAMES, first, second, gradients, strict=True)]
    return tuple(one[which] for which in range(3) for one in new)
```

```python
import functools

import jax
import jax.numpy as jnp
from jax import lax
from jax.experimental import pallas as pl
from jax.experimental.pallas import tpu as pltpu
from jax.sharding import PartitionSpec as P

NEG = -1e30
LOG2E = 1.4426950408889634
VMEM = 56 * 2**20
HEAD = 128
HEADS = 6
THETA = 10000
D = 512
FF = 2048
QKV = (HEADS + 2) * HEAD
ROW = HEADS * HEAD
FEED = 3 * FF
PART = 32
OUT = 48
DEVICES = 16
CHIPS = 8
HALF = HEAD // 2
STRIPE = 256
TILE = 512
BF16, F32 = jnp.bfloat16, jnp.float32
MESH = pl.DeviceIdType.MESH
NAMES = ("wq", "wk", "wv", "wo", "w_gate", "w_up", "w_down")


def _mm(a, b, ca=1, cb=0):
    return lax.dot_general(a, b, (((ca,), (cb,)), ((), ())), preferred_element_type=F32)


def _norm(h):
    wide = h.astype(F32)
    return wide, lax.rsqrt(jnp.mean(wide * wide, -1, keepdims=True) + 1e-6)


def _norm_back(wide, scale, by_normed):
    return by_normed * scale - wide * (scale * scale * scale * jnp.mean(by_normed * wide, -1, keepdims=True))


def _unfold_down(packed, out, devices):
    for j in range(devices):
        for p in range(4):
            out[pl.ds(PART * (4 * j + p), PART), :] = packed[pl.ds(PART * j, PART), pl.ds(D * p, D)]


def _fold_down(grad, out, row, col, devices):
    for j in range(devices):
        for p in range(4):
            out[pl.ds(pl.multiple_of(row + PART * j, PART), PART), pl.ds(col + D * p, D)] = lax.slice_in_dim(grad, PART * (4 * j + p), PART * (4 * j + p + 1))


def _fold_map(j):
    a, b, low = OUT * j, PART * j, OUT - PART
    yield pl.ds(a, PART), pl.ds(0, D), pl.ds(b, PART), pl.ds(0, D)
    for n in range(2):
        yield pl.ds(a + PART, low), pl.ds(n * STRIPE, STRIPE), pl.ds(b + low * n, low), pl.ds(D, STRIPE)


def _unfold_out(packed, out):
    for j in range(DEVICES):
        for rows, columns, there, columns_there in _fold_map(j):
            out[rows, columns] = packed[there, columns_there]


def _fold_out(grad, out):
    for j in range(DEVICES):
        for rows, columns, there, columns_there in _fold_map(j):
            out[there, columns_there] = grad[rows, columns].astype(out.dtype)


def _whole(shape):
    return pl.BlockSpec(shape, lambda *_: (0,) * len(shape))


def _call(body, grid, in_specs, out_specs, out_shape, scratch, flops, args, name):
    size = sum(a.size * a.dtype.itemsize for a in args)
    return pl.pallas_call(
        body, grid=grid, in_specs=in_specs, out_specs=out_specs, out_shape=out_shape, scratch_shapes=scratch, name=name,
        compiler_params=pltpu.CompilerParams(dimension_semantics=("arbitrary",) * len(grid), vmem_limit_bytes=VMEM),
        cost_estimate=pl.CostEstimate(flops=flops, bytes_accessed=size, transcendentals=0),
    )(*args)


def _project(h_ref, w_ref, near_ref, far_ref, q_ref, k_ref, v_ref):
    wide, scale = _norm(h_ref[...])
    t = _mm((wide * scale).astype(BF16), w_ref[...]).astype(BF16)
    near, far = near_ref[...], far_ref[...]
    heads = q_ref.shape[0]
    for n in range(heads + 1):
        x = t[:, n * HEAD : (n + 1) * HEAD].astype(F32)
        x = (x * near + pltpu.roll(x, HALF, 1) * far).astype(BF16)
        if n < heads:
            q_ref[n] = x
        else:
            k_ref[...] = x
    v_ref[...] = t[:, (heads + 1) * HEAD :]


def project(h, packed, at, near, far):
    t, d = h.shape
    heads = HEADS
    rows = lambda i: (i, 0)
    tokens = pl.BlockSpec((TILE, HEAD), rows)
    return _call(
        _project, (t // TILE,),
        [pl.BlockSpec((TILE, d), rows), pl.BlockSpec((d, QKV), lambda i: (0, at)), tokens, tokens],
        [pl.BlockSpec((heads, TILE, HEAD), lambda i: (0, i, 0)), tokens, tokens],
        [jax.ShapeDtypeStruct((heads, t, HEAD), BF16)] + [jax.ShapeDtypeStruct((t, HEAD), BF16)] * 2,
        [], 2 * t * d * QKV, (h, packed, near, far), "project")


def _heads(o_ref):
    return jnp.concatenate([o_ref[n] for n in range(o_ref.shape[0])], axis=1)


def _feed(o_ref, h_ref, gate_ref, up_ref, down_ref, out_ref, h1_ref, h2_ref, down_s, wo_s):
    @pl.when(pl.program_id(0) == 0)
    def _():
        _unfold_down(down_ref, down_s, DEVICES)
        _unfold_out(out_ref, wo_s)

    h1 = h_ref[...] + _mm(_heads(o_ref), wo_s[...]).astype(BF16)
    h1_ref[...] = h1
    wide, scale = _norm(h1)
    b = (wide * scale).astype(BF16)
    total = None
    for c in range(0, gate_ref.shape[1], TILE):
        gate = _mm(b, gate_ref[:, c : c + TILE])
        up = _mm(b, up_ref[:, c : c + TILE])
        part = _mm((gate * jax.nn.sigmoid(gate) * up).astype(BF16), down_s[c : c + TILE, :])
        total = part if total is None else total + part
    h2_ref[...] = h1 + total.astype(BF16)


def feed(o, h, packed, at_out):
    t, d = h.shape
    rows = pl.BlockSpec((TILE, d), lambda i: (i, 0))
    return _call(
        _feed, (t // TILE,),
        [pl.BlockSpec((HEADS, TILE, HEAD), lambda i: (0, i, 0)), rows] + [pl.BlockSpec((d, FF), lambda i, n=n: (0, n)) for n in range(3)]
        + [pl.BlockSpec((d, QKV), lambda i: (0, at_out))],
        [rows, rows], [jax.ShapeDtypeStruct((t, d), BF16)] * 2,
        [pltpu.VMEM((FF, d), BF16), pltpu.VMEM((ROW, d), BF16)], 2 * t * d * (ROW + FEED), (o, h, packed, packed, packed, packed), "feed")


def _join(o_ref, h_ref, out_ref, h1_ref, wo_s):
    @pl.when(pl.program_id(0) == 0)
    def _():
        _unfold_out(out_ref, wo_s)

    h1_ref[...] = h_ref[...] + _mm(_heads(o_ref), wo_s[...]).astype(BF16)


def join(o, h, packed, at_out):
    t, d = h.shape
    rows = pl.BlockSpec((TILE, d), lambda i: (i, 0))
    return _call(
        _join, (t // TILE,),
        [pl.BlockSpec((HEADS, TILE, HEAD), lambda i: (0, i, 0)), rows, pl.BlockSpec((d, QKV), lambda i: (0, at_out))],
        rows, jax.ShapeDtypeStruct((t, d), BF16), [pltpu.VMEM((ROW, d), BF16)], 2 * t * d * ROW, (o, h, packed), "join")


def _feed_back(h1_ref, dy_ref, gate_ref, up_ref, down_ref, *rest, more):
    more_ref, rest = (rest[0], rest[1:]) if more else (None, rest)
    by_h1_ref, grad_ref, b_s, bt_s, dyt_s, act_s, by_s, db_s, down_s = rest
    c = pl.program_id(0)
    t, d = h1_ref.shape
    tiles = t // TILE

    @pl.when(c == 0)
    def _():
        def prepare(i, _):
            here = pl.ds(pl.multiple_of(i * TILE, TILE), TILE)
            wide, scale = _norm(h1_ref[here, :])
            b = (wide * scale).astype(BF16)
            b_s[here, :] = b
            bt_s[:, here] = b.T
            dyt_s[:, here] = dy_ref[here, :].T
            db_s[here, :] = jnp.zeros((TILE, d), F32)
            return _

        lax.fori_loop(0, tiles, prepare, None)
        if more:
            grad_ref[:, FEED:] = more_ref[...]

    _unfold_down(down_ref, down_s, 4)

    def tile(i, _):
        here = pl.ds(pl.multiple_of(i * TILE, TILE), TILE)
        b = b_s[here, :]
        gate = _mm(b, gate_ref[...])
        up = _mm(b, up_ref[...])
        by_act = _mm(dy_ref[here, :], down_s[...], 1, 1).astype(BF16).astype(F32)
        soft = jax.nn.sigmoid(gate)
        silu = gate * soft
        act_s[here, :] = (silu * up).astype(BF16)
        by_up = (by_act * silu).astype(BF16)
        by_gate = (by_act * up * (soft + silu * (1 - soft))).astype(BF16)
        by_s[here, :TILE] = by_gate
        by_s[here, TILE:] = by_up
        db_s[here, :] += _mm(by_gate, gate_ref[...], 1, 1) + _mm(by_up, up_ref[...], 1, 1)
        return _

    lax.fori_loop(0, tiles, tile, None)
    here = pl.multiple_of(c * TILE, TILE)
    grad_ref[:, pl.ds(here, TILE)] = _mm(bt_s[...], by_s[:, :TILE]).astype(BF16)
    grad_ref[:, pl.ds(here + FF, TILE)] = _mm(bt_s[...], by_s[:, TILE:]).astype(BF16)
    _fold_down(_mm(dyt_s[...], act_s[...]).T.astype(BF16), grad_ref, c * HEAD, 2 * FF, 4)

    @pl.when(c == pl.num_programs(0) - 1)
    def _():
        def finish(i, _):
            here = pl.ds(pl.multiple_of(i * TILE, TILE), TILE)
            wide, scale = _norm(h1_ref[here, :])
            by_h1_ref[here, :] = dy_ref[here, :] + _norm_back(wide, scale, db_s[here, :].astype(BF16).astype(F32)).astype(BF16)
            return _

        lax.fori_loop(0, tiles, finish, None)


def feed_back(h1, dy, packed, more=None):
    t, d = h1.shape
    all_rows = _whole((t, d))
    columns = FEED + (0 if more is None else more.shape[1])
    extra = () if more is None else (more,)
    return _call(
        functools.partial(_feed_back, more=more is not None), (FF // TILE,),
        [all_rows, all_rows, pl.BlockSpec((d, TILE), lambda c: (0, c)), pl.BlockSpec((d, TILE), lambda c: (0, c + 4)),
         pl.BlockSpec((HEAD, FF), lambda c: (c, 2))] + [_whole(e.shape) for e in extra],
        [all_rows, _whole((d, columns))], [jax.ShapeDtypeStruct((t, d), BF16), jax.ShapeDtypeStruct((d, columns), BF16)],
        [pltpu.VMEM((t, d), BF16), pltpu.VMEM((d, t), BF16), pltpu.VMEM((d, t), BF16), pltpu.VMEM((t, TILE), BF16), pltpu.VMEM((t, 2 * TILE), BF16),
         pltpu.VMEM((t, d), F32), pltpu.VMEM((TILE, d), BF16)],
        2 * t * d * FF * 8, (h1, dy, packed, packed, packed, *extra), "feed_back")


def _join_back(dh_ref, o_ref, out_ref, by_o_ref, delta_ref, grad_ref, wo_s, sum_s):
    i = pl.program_id(0)

    @pl.when(i == 0)
    def _():
        _unfold_out(out_ref, wo_s)
        sum_s[...] = jnp.zeros_like(sum_s)

    dh = dh_ref[...]
    by_o = _mm(dh, wo_s[...], 1, 1).astype(BF16)
    for n in range(o_ref.shape[0]):
        o, by = o_ref[n], by_o[:, n * HEAD : (n + 1) * HEAD]
        by_o_ref[n] = by
        delta_ref[n : n + 1, :] = (o.astype(F32) * by.astype(F32)).T.sum(axis=0, keepdims=True)
        sum_s[n * HEAD : (n + 1) * HEAD, :] += _mm(o.T, dh)

    @pl.when(i == pl.num_programs(0) - 1)
    def _():
        _fold_out(sum_s, grad_ref)


def join_back(dh, o, packed, at_out):
    t, d = dh.shape
    heads = pl.BlockSpec((HEADS, TILE, HEAD), lambda i: (0, i, 0))
    return _call(
        _join_back, (t // TILE,),
        [pl.BlockSpec((TILE, d), lambda i: (i, 0)), heads, pl.BlockSpec((d, QKV), lambda i: (0, at_out))],
        [heads, pl.BlockSpec((HEADS, TILE), lambda i: (0, i)), _whole((d, ROW))],
        [jax.ShapeDtypeStruct((HEADS, t, HEAD), BF16), jax.ShapeDtypeStruct((HEADS, t), F32), jax.ShapeDtypeStruct((d, ROW), BF16)],
        [pltpu.VMEM((ROW, d), BF16), pltpu.VMEM((ROW, d), F32)], 4 * t * d * ROW, (dh, o, packed), "join_back")


def _project_back(dq_ref, dk_ref, dv_ref, near_ref, far_ref, h_ref, by_out_ref, *rest, states):
    if states:
        dh1_ref, w_ref, dh_ref, grad_ref, sum_s = rest
    else:
        grad_ref, sum_s = rest
    i = pl.program_id(0)

    @pl.when(i == 0)
    def _():
        sum_s[...] = jnp.zeros_like(sum_s)
        grad_ref[:, QKV:] = by_out_ref[...]

    near, far = near_ref[...], far_ref[...]
    parts = []
    for n in range(dq_ref.shape[0] + 1):
        x = (dq_ref[n] if n < dq_ref.shape[0] else dk_ref[...]).astype(F32)
        parts.append((x * near - pltpu.roll(x, HALF, 1) * far).astype(BF16))
    by = jnp.concatenate(parts + [dv_ref[...]], axis=1)
    wide, scale = _norm(h_ref[...])
    a = (wide * scale).astype(BF16)
    sum_s[...] += _mm(a.T, by)
    if states:
        da = _mm(by, w_ref[...], 1, 1).astype(BF16).astype(F32)
        dh_ref[...] = dh1_ref[...] + _norm_back(wide, scale, da).astype(BF16)

    @pl.when(i == pl.num_programs(0) - 1)
    def _():
        grad_ref[:, :QKV] = sum_s[...].astype(BF16)


def project_back(dq, dk, dv, near, far, h, by_out, dh1=None, packed=None, at=None):
    t, d = h.shape
    rows = lambda i: (i, 0)
    tokens, states = pl.BlockSpec((TILE, HEAD), rows), pl.BlockSpec((TILE, d), rows)
    args = [dq, dk, dv, near, far, h, by_out]
    specs = [pl.BlockSpec((HEADS, TILE, HEAD), lambda i: (0, i, 0)), tokens, tokens, tokens, tokens, states, _whole((d, ROW))]
    outs, shapes = [_whole((d, QKV + ROW))], [jax.ShapeDtypeStruct((d, QKV + ROW), BF16)]
    if dh1 is not None:
        args += [dh1, packed]
        specs += [states, pl.BlockSpec((d, QKV), lambda i: (0, at))]
        outs, shapes = [states] + outs, [jax.ShapeDtypeStruct((t, d), BF16)] + shapes
    return _call(functools.partial(_project_back, states=dh1 is not None), (t // TILE,), specs, outs, shapes,
                 [pltpu.VMEM((d, QKV), F32)], 2 * t * d * QKV * (1 if dh1 is None else 2), args, "project_back")


def _attend(q_ref, k_ref, v_ref, o_ref, lse_ref, top_s, mix_s, *, scale):
    i = pl.program_id(0)
    heads, size, _ = q_ref.shape
    e = scale * LOG2E
    ones = jnp.ones((mix_s.shape[1] - HEAD, size), BF16)
    top_s[...] = jnp.full(top_s.shape, NEG, F32)
    mix_s[...] = jnp.zeros(mix_s.shape, F32)

    def block(j, own):
        here = pl.ds(pl.multiple_of(j * size, size), size)
        scores = [_mm(k_ref[here, :], q_ref[n], 1, 1) for n in range(heads)]
        seen = lax.broadcasted_iota(jnp.int32, (size, size), 1) >= lax.broadcasted_iota(jnp.int32, (size, size), 0) if own else None
        weights, keeps = [], []
        for n, s in enumerate(scores):
            if own:
                s = jnp.where(seen, s, 2 * NEG)
            old = top_s[n : n + 1, :]
            top = jnp.maximum(old, s.max(axis=0, keepdims=True))
            top_s[n : n + 1, :] = top
            weights.append(jnp.exp2((s - top) * e).astype(BF16))
            keeps.append(jnp.exp2((old - top) * e))
        values = jnp.concatenate([v_ref[here, :].T, ones], axis=0)
        for n in range(heads):
            mix_s[n] = mix_s[n] * keeps[n] + _mm(values, weights[n])

    lax.fori_loop(0, i, lambda j, _: block(j, False), None)
    block(i, True)
    for n in range(heads):
        total = mix_s[n, HEAD : HEAD + 1, :]
        o_ref[n] = (mix_s[n, :HEAD, :] * (1 / total)).T.astype(BF16)
        lse_ref[n : n + 1, :] = top_s[n : n + 1, :] * scale + jnp.log(total)


def attended(q, k, v):
    heads, t, _ = q.shape
    queries, keys = pl.BlockSpec((heads, TILE, HEAD), lambda i: (0, i, 0)), _whole((t, HEAD))
    return _call(
        functools.partial(_attend, scale=HEAD**-0.5), (t // TILE,), [queries, keys, keys],
        [queries, pl.BlockSpec((heads, TILE), lambda i: (0, i))],
        [jax.ShapeDtypeStruct(q.shape, BF16), jax.ShapeDtypeStruct((heads, t), F32)],
        [pltpu.VMEM((heads, TILE), F32), pltpu.VMEM((heads, HEAD + 8, TILE), F32)], 2 * heads * t * t * HEAD, (q, k, v), "attended")


def _attend_back(q_ref, k_ref, v_ref, do_ref, lse_ref, delta_ref, dq_ref, dk_ref, dv_ref, dq_s, dk_s, dv_s, *, scale, keys):
    i = pl.program_id(0)
    heads, size, _ = q_ref.shape
    e = scale * LOG2E
    pairs = range(0, heads, 2)

    @pl.when(i == 0)
    def _():
        dk_s[...] = jnp.zeros_like(dk_s)
        dv_s[...] = jnp.zeros_like(dv_s)

    dq_s[...] = jnp.zeros_like(dq_s)
    side = lambda ref, n: jnp.concatenate([ref[n : n + 1, :], ref[n + 1 : n + 2, :]], axis=1)
    lses, deltas = [side(lse_ref, n) * LOG2E for n in pairs], [side(delta_ref, n) for n in pairs]
    whole = lax.div(i * size, keys)
    wide = 2 * size

    def block(j, own):
        here = pl.ds(pl.multiple_of(j * keys, keys), keys)
        qs = [q_ref[n : n + 2].reshape(wide, HEAD) for n in pairs]
        dos = [do_ref[n : n + 2].reshape(wide, HEAD) for n in pairs]
        scores = [_mm(k_ref[here, :], x, 1, 1) for x in qs]
        dps = [_mm(v_ref[here, :], x, 1, 1) for x in dos]
        if own:
            place = lax.rem(lax.broadcasted_iota(jnp.int32, (keys, wide), 1), size) - lax.broadcasted_iota(jnp.int32, (keys, wide), 0)
            seen = place >= j * keys - i * size
        for n, s in enumerate(scores):
            p = jnp.exp2(s * e - lses[n])
            if own:
                p = jnp.where(seen, p, 0.0)
            ds = (p * (dps[n] - deltas[n])).astype(BF16)
            dv_s[here, :] += _mm(p.astype(BF16), dos[n])
            dk_s[here, :] += _mm(ds, qs[n])
            dq_s[n] += _mm(k_ref[here, :].T, ds)

    lax.fori_loop(0, whole, lambda j, _: block(j, False), None)
    block(whole, True)
    for n in pairs:
        dq = (dq_s[n // 2] * scale).T.astype(BF16)
        dq_ref[n], dq_ref[n + 1] = dq[:size], dq[size:]

    @pl.when(i == pl.num_programs(0) - 1)
    def _():
        dk_ref[...] = (dk_s[...] * scale).astype(BF16)
        dv_ref[...] = dv_s[...].astype(BF16)


def attended_back(q, k, v, by_o, lse, delta):
    heads, t, _ = q.shape
    size = STRIPE
    queries, keys = pl.BlockSpec((heads, size, HEAD), lambda i: (0, i, 0)), _whole((t, HEAD))
    stats = pl.BlockSpec((heads, size), lambda i: (0, i))
    return _call(
        functools.partial(_attend_back, scale=HEAD**-0.5, keys=TILE), (t // size,), [queries, keys, keys, queries, stats, stats],
        [queries, keys, keys], [jax.ShapeDtypeStruct(a.shape, BF16) for a in (q, k, v)],
        [pltpu.VMEM((heads // 2, HEAD, 2 * size), F32), pltpu.VMEM((t, HEAD), F32), pltpu.VMEM((t, HEAD), F32)],
        5 * heads * t * t * HEAD, (q, k, v, by_o, lse, delta), "attended_back")


def turns(tokens):
    half = HALF
    angle = jnp.arange(tokens, dtype=F32)[:, None] * THETA ** (-jnp.arange(half, dtype=F32) / half)
    cos, sin = jnp.cos(angle), jnp.sin(angle)
    return jnp.concatenate([cos, cos], 1), jnp.concatenate([-sin, sin], 1)


def _place():
    me = lax.axis_index("dp")
    return me, lax.div(me, 2), lax.rem(me, 2)


def _meet(devices):
    barrier = pltpu.get_barrier_semaphore()
    for device in devices:
        pl.semaphore_signal(barrier, inc=1, device_id={"dp": device}, device_id_type=MESH)
    pl.semaphore_wait(barrier, len(devices))


def _send(source, target, send, recv, device):
    return pltpu.make_async_remote_copy(src_ref=source, dst_ref=target, send_sem=send, recv_sem=recv, device_id={"dp": device}, device_id_type=MESH)


def _rows(device):
    return pl.ds(pl.multiple_of(device * PART, PART), PART)


def _remote_call(body, number, out_shape, scratch, args, name):
    spec = pl.BlockSpec(memory_space=pltpu.VMEM)
    return pl.pallas_call(
        body, out_shape=out_shape, in_specs=[spec] * len(args), out_specs=spec, scratch_shapes=scratch, name=name,
        compiler_params=pltpu.CompilerParams(collective_id=number, has_side_effects=True, vmem_limit_bytes=VMEM),
        cost_estimate=pl.CostEstimate(flops=10**10, bytes_accessed=2 * 2**20, transcendentals=0),
    )(*args)


def _gather(x_ref, o_ref, send, recv, pass_send, pass_recv):
    me, chip, core = _place()
    other = me + 1 - 2 * core
    away = [lax.rem(chip + k, CHIPS) * 2 + core for k in range(CHIPS)]
    _meet([other] + away[1:])
    copies = [_send(x_ref, o_ref.at[_rows(me), :], send.at[k], recv.at[k], away[k]) for k in range(1, CHIPS)]
    passed = [_send(x_ref, o_ref.at[_rows(me), :], pass_send.at[0], pass_recv.at[0], other)]
    for copy in copies + passed:
        copy.start()
    o_ref[_rows(me), :] = x_ref[...]
    for k in range(1, CHIPS):
        copies[k - 1].wait_recv()
        block = o_ref.at[_rows(away[CHIPS - k]), :]
        passed.append(_send(block, block, pass_send.at[k], pass_recv.at[k], other))
        passed[k].start()
    for copy in copies:
        copy.wait_send()
    for copy in passed:
        copy.wait()


def gathered(x):
    sems = pltpu.SemaphoreType.DMA((CHIPS,))
    return _remote_call(_gather, 1, jax.ShapeDtypeStruct((DEVICES * PART, x.shape[1]), BF16), [sems] * 4, (x,), "gathered")


def _scatter(g_ref, o_ref, near_s, sent_s, far_s, pair_send, pair_recv, send, recv):
    me, chip, core = _place()
    other = me + 1 - 2 * core
    chips = [lax.rem(chip + k, CHIPS) * 2 for k in range(CHIPS)]
    _meet([other] + [c + core for c in chips[1:]])
    pairs = [_send(g_ref.at[_rows(chips[k] + 1 - core), :], near_s.at[k], pair_send.at[k], pair_recv.at[k], other) for k in range(CHIPS)]
    order = [*range(1, CHIPS), 0]
    for k in order:
        pairs[k].start()
    copies = []
    for k in order:
        pairs[k].wait_recv()
        both = g_ref[_rows(chips[k] + core), :].astype(F32) + near_s[k].astype(F32)
        if k == 0:
            break
        sent_s[k] = both.astype(BF16)
        copies.append(_send(sent_s.at[k], far_s.at[k], send.at[k], recv.at[k], chips[k] + core))
        copies[-1].start()
    for k in range(1, CHIPS):
        copies[k - 1].wait_recv()
        both = both + far_s[k].astype(F32)
    o_ref[...] = both.astype(BF16)
    for copy in pairs + copies:
        copy.wait_send()


def scattered(g):
    sems, blocks = pltpu.SemaphoreType.DMA((CHIPS,)), pltpu.VMEM((CHIPS, PART, g.shape[1]), BF16)
    return _remote_call(_scatter, 2, jax.ShapeDtypeStruct((PART, g.shape[1]), BF16), [blocks] * 3 + [sems] * 4, (g,), "scattered")


def _squares(*refs):
    pieces, (o_ref, own_s, all_s, send, recv) = refs[:-5], refs[-5:]
    me, _, _ = _place()
    away = [lax.rem(me + k, DEVICES) for k in range(DEVICES)]
    total = 0.0
    for ref in pieces:
        g = ref[...].astype(F32)
        total = total + jnp.sum(g * g)
    own_s[...] = jnp.full(own_s.shape, total, F32)
    _meet(away[1:])
    copies = [_send(own_s, all_s.at[me], send.at[k], recv.at[k], away[k]) for k in range(1, DEVICES)]
    for copy in copies:
        copy.start()
    all_s[me] = own_s[...]
    for copy in copies:
        copy.wait()
    o_ref[...] = all_s[...].sum(axis=0)


def squares(*pieces):
    tile, sems = (8, HEAD), pltpu.SemaphoreType.DMA((DEVICES,))
    return _remote_call(_squares, 3, jax.ShapeDtypeStruct(tile, F32), [pltpu.VMEM(tile, F32), pltpu.VMEM((DEVICES, *tile), F32), sems, sems], pieces, "squares")


def _pack(wq, wk, wv, wo, gate, up, down, first, layer0, layer1):
    def projections(out, at, n):
        for w in (wq, wk, wv):
            out[:, pl.ds(at, w.shape[2])] = w[n]
            at += w.shape[2]

    def rest(out, at, n):
        out[:, :FF] = gate[n]
        out[:, FF : 2 * FF] = up[n]
        for p in range(4):
            out[:, pl.ds(2 * FF + D * p, D)] = down[n, PART * p : PART * p + PART, :]
        for rows, columns, there, columns_there in _fold_map(0):
            out[there, pl.ds(at + columns_there.start, columns_there.size)] = wo[n, rows, columns]
        out[:, at + ROW :] = jnp.zeros((PART, STRIPE), BF16)

    projections(first, 0, 0)
    rest(layer0, FEED + QKV, 0)
    projections(layer0, FEED, 1)
    rest(layer1, FEED, 1)


def packed_weights(weights):
    shapes = [jax.ShapeDtypeStruct((PART, n), BF16) for n in (QKV, FEED + 2 * QKV, FEED + QKV)]
    return _call(_pack, (1,), [_whole(w.shape) for w in weights], [_whole(s.shape) for s in shapes], shapes, [], 10**6, weights, "pack")


def _adamw(*refs, count):
    (total_ref, feed1_ref, both_ref, rest0_ref), refs = refs[:4], refs[4:]
    old, new = [refs[n : n + 7] for n in range(0, 21, 7)], [refs[n : n + 7] for n in range(21, 42, 7)]
    factor = jnp.minimum(1.0, 0.5 * lax.rsqrt(total_ref[:1, :1] / count + 1e-30))

    def update(name, layer, rows, columns, grad):
        i = NAMES.index(name)
        g = grad.astype(F32) * factor
        w, m, v = (one[i][layer, rows, columns] for one in old)
        w = w.astype(F32)
        m = 0.9 * m + 0.1 * g
        v = 0.95 * v + 0.05 * g * g
        step = m * lax.rsqrt(v + 1e-8) + 0.1 * w
        for one, value in zip(new, ((w - 0.02 * step).astype(BF16), m, v)):
            one[i][layer, rows, columns] = value

    every = slice(None)
    for layer, feed, rest, at in ((0, both_ref, rest0_ref, 0), (1, feed1_ref, both_ref, FEED)):
        for name in ("wq", "wk", "wv"):
            width = old[0][NAMES.index(name)].shape[2]
            update(name, layer, every, every, rest[:, pl.ds(at, width)])
            at += width
        for rows, columns, there, columns_there in _fold_map(0):
            update("wo", layer, rows, columns, rest[there, pl.ds(at + columns_there.start, columns_there.size)])
        update("w_gate", layer, every, every, feed[:, :FF])
        update("w_up", layer, every, every, feed[:, FF : 2 * FF])
        for p in range(4):
            update("w_down", layer, pl.ds(PART * p, PART), every, feed[:, pl.ds(2 * FF + D * p, D)])


def adamw(total, feed1, both, rest0, count, weights, m, v):
    args = (total, feed1, both, rest0, *weights, *m, *v)
    shapes = [jax.ShapeDtypeStruct(a.shape, a.dtype) for a in args[4:]]
    return _call(functools.partial(_adamw, count=count), (1,), [_whole(a.shape) for a in args], [_whole(s.shape) for s in shapes], shapes, [],
                 10**7, args, "adamw")


def solution(mesh):
    def gather(part):
        return lax.all_gather(part, "dp", axis=0, tiled=True)

    def scatter(gradient):
        return lax.psum_scatter(gradient, "dp", scatter_dimension=0, tiled=True)

    def step(x, dy, *arrays):
        weights, m, v = (arrays[i : i + 7] for i in (0, 7, 14))
        x, dy = x[0], dy[0]
        first, layer0, layer1 = packed_weights(weights)
        layer0, layer1, first = gather(layer0), gather(layer1), gathered(first)
        near, far = turns(x.shape[0])

        q0, k0, v0 = project(x, first, 0, near, far)
        o0, lse0 = attended(q0, k0, v0)
        mid0, h = feed(o0, x, layer0, 7)
        q1, k1, v1 = project(h, layer0, 6, near, far)
        o1, lse1 = attended(q1, k1, v1)
        mid1 = join(o1, h, layer1, 6)

        by_mid, feed1 = feed_back(mid1, dy, layer1)
        feed1 = scatter(feed1)
        by_o, delta, by_out = join_back(by_mid, o1, layer1, 6)
        dq, dk, dv = attended_back(q1, k1, v1, by_o, lse1, delta)
        by_h, rest1 = project_back(dq, dk, dv, near, far, h, by_out, by_mid, layer0, 6)

        by_mid, both = feed_back(mid0, by_h, layer0, rest1)
        feed1, both = lax.optimization_barrier((feed1, both))
        both = scatter(both)
        by_o, delta, by_out = join_back(by_mid, o0, layer0, 7)
        dq, dk, dv = attended_back(q0, k0, v0, by_o, lse0, delta)
        (rest0,) = project_back(dq, dk, dv, near, far, x, by_out)
        rest0 = scattered(rest0)

        total = squares(feed1, both, rest0)
        count = DEVICES * sum(g.size for g in (feed1, both, rest0))
        return tuple(adamw(total, feed1, both, rest0, count, weights, m, v))

    states, cut = P(("rep", "dp"), None, None), P(None, "dp", None)
    return jax.shard_map(
        step,
        mesh=mesh,
        in_specs=(states, states) + (cut,) * 21,
        out_specs=(P("rep", "dp", None),) * 21,
        check_vma=False,
    )
```

```python
import functools

import jax
import jax.numpy as jnp
from jax import lax
from jax.experimental import pallas as pl
from jax.experimental.pallas import tpu as pltpu
from jax.sharding import PartitionSpec as P

NEG = -1e30
LOG2E = 1.4426950408889634
VMEM = 56 * 2**20
HEAD = 128
HEADS = 6
THETA = 10000
D = 512
FF = 2048
QKV = (HEADS + 2) * HEAD
ROW = HEADS * HEAD
FEED = 3 * FF
PART = 32
OUT = 48
DEVICES = 16
CHIPS = 8
HALF = HEAD // 2
STRIPE = 256
TILE = 512
BF16, F32 = jnp.bfloat16, jnp.float32
MESH = pl.DeviceIdType.MESH
NAMES = ("wq", "wk", "wv", "wo", "w_gate", "w_up", "w_down")


def _mm(a, b, ca=1, cb=0):
    return lax.dot_general(a, b, (((ca,), (cb,)), ((), ())), preferred_element_type=F32)


def _norm(h):
    wide = h.astype(F32)
    return wide, lax.rsqrt(jnp.mean(wide * wide, -1, keepdims=True) + 1e-6)


def _norm_back(wide, scale, by_normed):
    return by_normed * scale - wide * (scale * scale * scale * jnp.mean(by_normed * wide, -1, keepdims=True))


def _unfold_down(packed, out, devices):
    for j in range(devices):
        for p in range(4):
            out[pl.ds(PART * (4 * j + p), PART), :] = packed[pl.ds(PART * j, PART), pl.ds(D * p, D)]


def _fold_down(grad, out, row, col, devices):
    for j in range(devices):
        for p in range(4):
            out[pl.ds(pl.multiple_of(row + PART * j, PART), PART), pl.ds(col + D * p, D)] = lax.slice_in_dim(grad, PART * (4 * j + p), PART * (4 * j + p + 1))


def _fold_map(j):
    a, b, low = OUT * j, PART * j, OUT - PART
    yield pl.ds(a, PART), pl.ds(0, D), pl.ds(b, PART), pl.ds(0, D)
    for n in range(2):
        yield pl.ds(a + PART, low), pl.ds(n * STRIPE, STRIPE), pl.ds(b + low * n, low), pl.ds(D, STRIPE)


def _unfold_out(packed, out):
    for j in range(DEVICES):
        for rows, columns, there, columns_there in _fold_map(j):
            out[rows, columns] = packed[there, columns_there]


def _fold_out(grad, out):
    for j in range(DEVICES):
        for rows, columns, there, columns_there in _fold_map(j):
            out[there, columns_there] = grad[rows, columns].astype(out.dtype)


def _whole(shape):
    return pl.BlockSpec(shape, lambda *_: (0,) * len(shape))


def _call(body, grid, in_specs, out_specs, out_shape, scratch, flops, args, name, number=None):
    size = sum(a.size * a.dtype.itemsize for a in args)
    return pl.pallas_call(
        body, grid=grid, in_specs=in_specs, out_specs=out_specs, out_shape=out_shape, scratch_shapes=scratch, name=name,
        compiler_params=pltpu.CompilerParams(dimension_semantics=("arbitrary",) * len(grid), vmem_limit_bytes=VMEM, collective_id=number,
                                             has_side_effects=number is not None),
        cost_estimate=pl.CostEstimate(flops=flops, bytes_accessed=size, transcendentals=0),
    )(*args)


def _project_tile(h, w, near, far, rows, q_ref, k_ref, v_ref):
    wide, scale = _norm(h)
    t = _mm((wide * scale).astype(BF16), w).astype(BF16)
    heads = q_ref.shape[0]
    for n in range(heads + 1):
        x = t[:, n * HEAD : (n + 1) * HEAD].astype(F32)
        x = (x * near + pltpu.roll(x, HALF, 1) * far).astype(BF16)
        if n < heads:
            q_ref[n, rows, :] = x
        else:
            k_ref[rows, :] = x
    v_ref[rows, :] = t[:, (heads + 1) * HEAD :]


def _heads(o_ref, rows=slice(None)):
    return jnp.concatenate([o_ref[n, rows, :] for n in range(o_ref.shape[0])], axis=1)


def _feed_tile(rows, o_ref, h_ref, w_ref, h1_ref, h2_ref, down_s, wo_s):
    h1 = h_ref[rows, :] + _mm(_heads(o_ref, rows), wo_s[...]).astype(BF16)
    h1_ref[rows, :] = h1
    wide, scale = _norm(h1)
    b = (wide * scale).astype(BF16)
    total = None
    for c in range(0, FF, TILE):
        gate = _mm(b, w_ref[:, pl.ds(c, TILE)])
        up = _mm(b, w_ref[:, pl.ds(FF + c, TILE)])
        part = _mm((gate * jax.nn.sigmoid(gate) * up).astype(BF16), down_s[pl.ds(c, TILE), :])
        total = part if total is None else total + part
    h2_ref[rows, :] = h1 + total.astype(BF16)


def _feed_back(h1_ref, dy_ref, gate_ref, up_ref, down_ref, by_h1_ref, grad_ref, b_s, bt_s, dyt_s, act_s, by_s, db_s, down_s):
    c = pl.program_id(0)
    t, d = h1_ref.shape
    tiles = t // TILE

    @pl.when(c == 0)
    def _():
        def prepare(i, _):
            here = pl.ds(pl.multiple_of(i * TILE, TILE), TILE)
            wide, scale = _norm(h1_ref[here, :])
            b = (wide * scale).astype(BF16)
            b_s[here, :] = b
            bt_s[:, here] = b.T
            dyt_s[:, here] = dy_ref[here, :].T
            db_s[here, :] = jnp.zeros((TILE, d), F32)
            return _

        lax.fori_loop(0, tiles, prepare, None)

    _unfold_down(down_ref, down_s, 4)

    pieces = [pl.ds(i * TILE, TILE) for i in range(tiles)]
    dots = []
    for here in pieces:
        b = b_s[here, :]
        dots.append((_mm(b, gate_ref[...]), _mm(b, up_ref[...]), _mm(dy_ref[here, :], down_s[...], 1, 1)))
    for here, (gate, up, by_act) in zip(pieces, dots):
        by_act = by_act.astype(BF16).astype(F32)
        soft = jax.nn.sigmoid(gate)
        silu = gate * soft
        act_s[here, :] = (silu * up).astype(BF16)
        by_s[here, TILE:] = (by_act * silu).astype(BF16)
        by_s[here, :TILE] = (by_act * up * (soft + silu * (1 - soft))).astype(BF16)
    for here in pieces:
        db_s[here, :] += _mm(by_s[here, :TILE], gate_ref[...], 1, 1) + _mm(by_s[here, TILE:], up_ref[...], 1, 1)
    here = pl.multiple_of(c * TILE, TILE)
    grad_ref[:, pl.ds(here, TILE)] = _mm(bt_s[...], by_s[:, :TILE]).astype(BF16)
    grad_ref[:, pl.ds(here + FF, TILE)] = _mm(bt_s[...], by_s[:, TILE:]).astype(BF16)
    _fold_down(_mm(dyt_s[...], act_s[...]).T.astype(BF16), grad_ref, c * HEAD, 2 * FF, 4)

    @pl.when(c == pl.num_programs(0) - 1)
    def _():
        def finish(i, _):
            here = pl.ds(pl.multiple_of(i * TILE, TILE), TILE)
            wide, scale = _norm(h1_ref[here, :])
            by_h1_ref[here, :] = dy_ref[here, :] + _norm_back(wide, scale, db_s[here, :].astype(BF16).astype(F32)).astype(BF16)
            return _

        lax.fori_loop(0, tiles, finish, None)


def feed_back(h1, dy, packed):
    t, d = h1.shape
    all_rows = _whole((t, d))
    return _call(
        _feed_back, (FF // TILE,),
        [all_rows, all_rows, pl.BlockSpec((d, TILE), lambda c: (0, c)), pl.BlockSpec((d, TILE), lambda c: (0, c + 4)),
         pl.BlockSpec((HEAD, FF), lambda c: (c, 2))],
        [all_rows, _whole((d, FEED))], [jax.ShapeDtypeStruct((t, d), BF16), jax.ShapeDtypeStruct((d, FEED), BF16)],
        [pltpu.VMEM((t, d), BF16), pltpu.VMEM((d, t), BF16), pltpu.VMEM((d, t), BF16), pltpu.VMEM((t, TILE), BF16), pltpu.VMEM((t, 2 * TILE), BF16),
         pltpu.VMEM((t, d), F32), pltpu.VMEM((TILE, d), BF16)],
        2 * t * d * FF * 8, (h1, dy, packed, packed, packed), "feed_back")


def _join_back(dh_ref, o_ref, out_ref, by_o_ref, delta_ref, grad_ref, wo_s, sum_s):
    i = pl.program_id(0)

    @pl.when(i == 0)
    def _():
        _unfold_out(out_ref, wo_s)
        sum_s[...] = jnp.zeros_like(sum_s)

    dh = dh_ref[...]
    by_o = _mm(dh, wo_s[...], 1, 1).astype(BF16)
    for n in range(o_ref.shape[0]):
        o, by = o_ref[n], by_o[:, n * HEAD : (n + 1) * HEAD]
        by_o_ref[n] = by
        delta_ref[n : n + 1, :] = (o.astype(F32) * by.astype(F32)).T.sum(axis=0, keepdims=True)
        sum_s[n * HEAD : (n + 1) * HEAD, :] += _mm(o.T, dh)

    @pl.when(i == pl.num_programs(0) - 1)
    def _():
        _fold_out(sum_s, grad_ref)


def join_back(dh, o, packed, at_out):
    t, d = dh.shape
    heads = pl.BlockSpec((HEADS, TILE, HEAD), lambda i: (0, i, 0))
    return _call(
        _join_back, (t // TILE,),
        [pl.BlockSpec((TILE, d), lambda i: (i, 0)), heads, pl.BlockSpec((d, QKV), lambda i: (0, at_out))],
        [heads, pl.BlockSpec((HEADS, TILE), lambda i: (0, i)), _whole((d, ROW))],
        [jax.ShapeDtypeStruct((HEADS, t, HEAD), BF16), jax.ShapeDtypeStruct((HEADS, t), F32), jax.ShapeDtypeStruct((d, ROW), BF16)],
        [pltpu.VMEM((ROW, d), BF16), pltpu.VMEM((ROW, d), F32)], 4 * t * d * ROW, (dh, o, packed), "join_back")


def _project_back(dq_ref, dk_ref, dv_ref, near_ref, far_ref, h_ref, by_out_ref, *rest, states):
    if states:
        dh1_ref, w_ref, dh_ref, grad_ref, sum_s = rest
    else:
        grad_ref, sum_s = rest
    i = pl.program_id(0)

    @pl.when(i == 0)
    def _():
        sum_s[...] = jnp.zeros_like(sum_s)
        grad_ref[:, QKV:] = by_out_ref[...]

    near, far = near_ref[...], far_ref[...]
    parts = []
    for n in range(dq_ref.shape[0] + 1):
        x = (dq_ref[n] if n < dq_ref.shape[0] else dk_ref[...]).astype(F32)
        parts.append((x * near - pltpu.roll(x, HALF, 1) * far).astype(BF16))
    by = jnp.concatenate(parts + [dv_ref[...]], axis=1)
    wide, scale = _norm(h_ref[...])
    a = (wide * scale).astype(BF16)
    sum_s[...] += _mm(a.T, by)
    if states:
        da = _mm(by, w_ref[...], 1, 1).astype(BF16).astype(F32)
        dh_ref[...] = dh1_ref[...] + _norm_back(wide, scale, da).astype(BF16)

    @pl.when(i == pl.num_programs(0) - 1)
    def _():
        grad_ref[:, :QKV] = sum_s[...].astype(BF16)


def project_back(dq, dk, dv, near, far, h, by_out, dh1=None, packed=None, at=None):
    t, d = h.shape
    rows = lambda i: (i, 0)
    tokens, states = pl.BlockSpec((TILE, HEAD), rows), pl.BlockSpec((TILE, d), rows)
    args = [dq, dk, dv, near, far, h, by_out]
    specs = [pl.BlockSpec((HEADS, TILE, HEAD), lambda i: (0, i, 0)), tokens, tokens, tokens, tokens, states, _whole((d, ROW))]
    outs, shapes = [_whole((d, QKV + ROW))], [jax.ShapeDtypeStruct((d, QKV + ROW), BF16)]
    if dh1 is not None:
        args += [dh1, packed]
        specs += [states, pl.BlockSpec((d, QKV), lambda i: (0, at))]
        outs, shapes = [states] + outs, [jax.ShapeDtypeStruct((t, d), BF16)] + shapes
    return _call(functools.partial(_project_back, states=dh1 is not None), (t // TILE,), specs, outs, shapes,
                 [pltpu.VMEM((d, QKV), F32)], 2 * t * d * QKV * (1 if dh1 is None else 2), args, "project_back")


def _attend_tile(i, rows, q_ref, k_ref, v_ref, o_ref, lse_ref, top_s, mix_s):
    heads, size = top_s.shape
    scale = HEAD**-0.5
    e = scale * LOG2E
    ones = jnp.ones((mix_s.shape[1] - HEAD, size), BF16)
    top_s[...] = jnp.full(top_s.shape, NEG, F32)
    mix_s[...] = jnp.zeros(mix_s.shape, F32)

    def block(j, own):
        here = pl.ds(pl.multiple_of(j * size, size), size)
        scores = [_mm(k_ref[here, :], q_ref[n, rows, :], 1, 1) for n in range(heads)]
        seen = lax.broadcasted_iota(jnp.int32, (size, size), 1) >= lax.broadcasted_iota(jnp.int32, (size, size), 0) if own else None
        weights, keeps = [], []
        for n, s in enumerate(scores):
            if own:
                s = jnp.where(seen, s, 2 * NEG)
            old = top_s[n : n + 1, :]
            top = jnp.maximum(old, s.max(axis=0, keepdims=True))
            top_s[n : n + 1, :] = top
            weights.append(jnp.exp2((s - top) * e).astype(BF16))
            keeps.append(jnp.exp2((old - top) * e))
        values = jnp.concatenate([v_ref[here, :].T, ones], axis=0)
        for n in range(heads):
            mix_s[n] = mix_s[n] * keeps[n] + _mm(values, weights[n])

    lax.fori_loop(0, i, lambda j, _: block(j, False), None)
    block(i, True)
    for n in range(heads):
        total = mix_s[n, HEAD : HEAD + 1, :]
        o_ref[n, rows, :] = (mix_s[n, :HEAD, :] * (1 / total)).T.astype(BF16)
        lse_ref[n : n + 1, rows] = top_s[n : n + 1, :] * scale + jnp.log(total)


ATTEND_SCRATCH = [pltpu.VMEM((HEADS, TILE), F32), pltpu.VMEM((HEADS, HEAD + 8, TILE), F32)]


def _attend_back(q_ref, k_ref, v_ref, do_ref, lse_ref, delta_ref, *rest, scale, scatter):
    i, last = pl.program_id(0), pl.num_programs(0) - 1
    if scatter:
        g_ref, dq_ref, dk_ref, dv_ref, r_ref, dq_s, dk_s, dv_s = rest[:8]
        starts, passes, ends = _scatter_phases(g_ref, r_ref, *rest[8:])
        pl.when(i == 0)(starts)
        pl.when(i == 1)(passes)
    else:
        dq_ref, dk_ref, dv_ref, dq_s, dk_s, dv_s = rest
    heads, size, _ = q_ref.shape
    e = scale * LOG2E
    pairs = range(0, heads, 2)

    @pl.when(i == 0)
    def _():
        dk_s[...] = jnp.zeros_like(dk_s)
        dv_s[...] = jnp.zeros_like(dv_s)

    dq_s[...] = jnp.zeros_like(dq_s)
    side = lambda ref, n: jnp.concatenate([ref[n : n + 1, :], ref[n + 1 : n + 2, :]], axis=1)
    lses, deltas = [side(lse_ref, n) * LOG2E for n in pairs], [side(delta_ref, n) for n in pairs]
    wide = 2 * size

    def block(j, own):
        here = pl.ds(pl.multiple_of(j * size, size), size)
        qs = [q_ref[n : n + 2].reshape(wide, HEAD) for n in pairs]
        dos = [do_ref[n : n + 2].reshape(wide, HEAD) for n in pairs]
        scores = [_mm(k_ref[here, :], x, 1, 1) for x in qs]
        dps = [_mm(v_ref[here, :], x, 1, 1) for x in dos]
        if own:
            seen = lax.rem(lax.broadcasted_iota(jnp.int32, (size, wide), 1), size) >= lax.broadcasted_iota(jnp.int32, (size, wide), 0)
        for n, s in enumerate(scores):
            p = jnp.exp2(s * e - lses[n])
            if own:
                p = jnp.where(seen, p, 0.0)
            ds = (p * (dps[n] - deltas[n])).astype(BF16)
            dv_s[here, :] += _mm(p.astype(BF16), dos[n])
            dk_s[here, :] += _mm(ds, qs[n])
            dq_s[n] += _mm(k_ref[here, :].T, ds)

    lax.fori_loop(0, i, lambda j, _: block(j, False), None)
    block(i, True)
    for n in pairs:
        dq = (dq_s[n // 2] * scale).T.astype(BF16)
        dq_ref[n], dq_ref[n + 1] = dq[:size], dq[size:]

    @pl.when(i == last)
    def _():
        dk_ref[...] = (dk_s[...] * scale).astype(BF16)
        dv_ref[...] = dv_s[...].astype(BF16)

    if scatter:
        pl.when(i == last)(ends)


def attended_back(q, k, v, by_o, lse, delta, gradient=None):
    heads, t, _ = q.shape
    size = TILE
    queries, keys = pl.BlockSpec((heads, size, HEAD), lambda i: (0, i, 0)), _whole((t, HEAD))
    stats = pl.BlockSpec((heads, size), lambda i: (0, i))
    specs, outs, shapes = [queries, keys, keys, queries, stats, stats], [queries, keys, keys], [jax.ShapeDtypeStruct(a.shape, BF16) for a in (q, k, v)]
    scratch = [pltpu.VMEM((heads // 2, HEAD, 2 * size), F32), pltpu.VMEM((t, HEAD), F32), pltpu.VMEM((t, HEAD), F32)]
    args = (q, k, v, by_o, lse, delta)
    if gradient is not None:
        shape = (PART, gradient.shape[1])
        args, specs, outs = (*args, gradient), specs + [_whole(gradient.shape)], outs + [_whole(shape)]
        shapes, scratch = shapes + [jax.ShapeDtypeStruct(shape, BF16)], scratch + _scatter_scratch(gradient)
    return _call(functools.partial(_attend_back, scale=HEAD**-0.5, scatter=gradient is not None), (t // size,), specs, outs, shapes, scratch,
                 5 * heads * t * t * HEAD, args, "attended_back", None if gradient is None else 4)


def turns(tokens):
    place = jnp.concatenate([jnp.arange(0, tokens, PART, dtype=F32), jnp.arange(PART, dtype=F32)])
    angle = place[:, None] * THETA ** (-jnp.arange(HALF, dtype=F32) / HALF)
    cos, sin = jnp.cos(angle), jnp.sin(angle)
    return jnp.concatenate([cos, cos], 1), jnp.concatenate([-sin, sin], 1)


def _turn_tables(cos_ref, sin_ref, near_ref, far_ref):
    runs = near_ref.shape[0] // PART
    cos, sin = cos_ref[runs:, :], sin_ref[runs:, :]
    for i in range(runs):
        rows = pl.ds(i * PART, PART)
        cos_i, sin_i = cos_ref[i : i + 1, :], sin_ref[i : i + 1, :]
        near_ref[rows, :] = cos_i * cos - sin_i * sin
        far_ref[rows, :] = sin_i * cos + cos_i * sin


def _place():
    me = lax.axis_index("dp")
    return me, lax.div(me, 2), lax.rem(me, 2)


def _meet(devices, meanwhile=lambda: None):
    barrier = pltpu.get_barrier_semaphore()
    for device in devices:
        pl.semaphore_signal(barrier, inc=1, device_id={"dp": device}, device_id_type=MESH)
    meanwhile()
    pl.semaphore_wait(barrier, len(devices))


def _send(source, target, send, recv, device):
    return pltpu.make_async_remote_copy(src_ref=source, dst_ref=target, send_sem=send, recv_sem=recv, device_id={"dp": device}, device_id_type=MESH)


def _rows(device):
    return pl.ds(pl.multiple_of(device * PART, PART), PART)


def _remote_call(body, number, out_shape, scratch, args, name):
    spec = pl.BlockSpec(memory_space=pltpu.VMEM)
    return pl.pallas_call(
        body, out_shape=out_shape, in_specs=[spec] * len(args), out_specs=jax.tree.map(lambda _: spec, out_shape), scratch_shapes=scratch, name=name,
        compiler_params=pltpu.CompilerParams(collective_id=number, has_side_effects=True, vmem_limit_bytes=VMEM),
        cost_estimate=pl.CostEstimate(flops=10**10, bytes_accessed=2 * 2**20, transcendentals=0),
    )(*args)


def _around():
    me, chip, core = _place()
    line = CHIPS // 2
    turned = lambda n: n + lax.div(n, line) * (3 * line - 1 - 2 * n)
    place = turned(chip)
    return me, me + 1 - 2 * core, lambda k: turned(lax.rem(place + k, CHIPS)) * 2 + core


def _ring(layer_ref, all_ref, ring_send, ring_recv, over_send, over_recv):
    me, other, ring = _around()
    half = layer_ref.shape[1] // 2
    steps = CHIPS - 1
    columns = lambda n: pl.ds(n * half if isinstance(n, int) else pl.multiple_of(n * half, half), half)
    block = lambda device, n: all_ref.at[_rows(device), columns(n)]
    sides = ((0, ring(1), 0), (1, ring(steps), 1))
    whole = _send(layer_ref, all_ref.at[_rows(me), :], over_send.at[2 * steps], over_recv.at[2 * steps], other)

    def half_of(n, lead):
        return (n + lead) % 2 if isinstance(n, int) else lax.rem(n + lead, 2)

    def on(way, n, source, target, neighbour):
        return _send(source, target, ring_send.at[way * steps + n], ring_recv.at[way * steps + n], neighbour)

    def over(way, n, got):
        return _send(got, got, over_send.at[way * steps + n], over_recv.at[way * steps + n], other)

    def start():
        for n in range(2):
            for way, neighbour, lead in sides:
                h = half_of(n, lead)
                on(way, n, layer_ref.at[:, columns(h)], block(me, h), neighbour).start()
        whole.start()
        all_ref[_rows(me), :] = layer_ref[...]

    def serve(n, onward=True):
        for way, neighbour, lead in sides:
            h = half_of(n, lead)
            far = n // 2 + 1 if isinstance(n, int) else lax.div(n, 2) + 1
            got = block(ring(far if way else CHIPS - far), h)
            on(way, n, got, got, neighbour).wait_recv()
            if onward:
                on(way, n + 2, got, got, neighbour).start()
            over(way, n, got).start()

    def finish():
        for n in range(steps):
            for way, neighbour, lead in sides:
                got = block(me, half_of(n, lead))
                on(way, n, got, got, neighbour).wait_send()
                over(way, n, got).wait()
        whole.wait()

    return start, serve, finish


def _begin(first_ref, layer_ref, x_ref, cos_ref, sin_ref, q_ref, k_ref, v_ref, o_ref, lse_ref, all_ref, near_ref, far_ref, w_s, top_s, mix_s,
           send, recv, pass_send, pass_recv, *sems):
    me, other, ring = _around()
    away = [ring(k) for k in range(CHIPS)]
    _meet([other] + away[1:])
    mine = w_s.at[_rows(me), :]
    copies = [_send(first_ref, mine, send.at[k], recv.at[k], away[k]) for k in range(1, CHIPS)]
    passed = [_send(first_ref, mine, pass_send.at[0], pass_recv.at[0], other)]
    for copy in copies + passed:
        copy.start()
    start, serve, finish = _ring(layer_ref, all_ref, *sems)
    start()
    w_s[_rows(me), :] = first_ref[...]
    _turn_tables(cos_ref, sin_ref, near_ref, far_ref)
    for k in range(1, CHIPS):
        copies[k - 1].wait_recv()
        got = w_s.at[_rows(away[CHIPS - k]), :]
        passed.append(_send(got, got, pass_send.at[k], pass_recv.at[k], other))
        passed[k].start()
    for copy in passed:
        copy.wait_recv()
    serve(0)

    def project_tile(i, _):
        _project_rest(i, x_ref, w_s, near_ref, far_ref, q_ref, k_ref, v_ref)

        @pl.when(i < 2)
        def _():
            serve(i + 1)

    tiles = x_ref.shape[0] // TILE
    lax.fori_loop(0, tiles, project_tile, None)

    def attend_tile(i, _):
        _attend_tile(i, pl.ds(pl.multiple_of(i * TILE, TILE), TILE), q_ref, k_ref, v_ref, o_ref, lse_ref, top_s, mix_s)
        pl.when(i < 2)(lambda: serve(i + 3))
        pl.when(i >= 2)(lambda: serve(i + 3, False))

    lax.fori_loop(0, tiles, attend_tile, None)
    for copy in copies + passed:
        copy.wait_send()
    finish()


def _project_rest(i, x_ref, w_ref, near_ref, far_ref, q_ref, k_ref, v_ref):
    rows = pl.ds(pl.multiple_of(i * TILE, TILE), TILE)
    _project_tile(x_ref[rows, :], w_ref[...], near_ref[rows, :], far_ref[rows, :], rows, q_ref, k_ref, v_ref)


def _attention_shapes(t):
    tokens, heads = jax.ShapeDtypeStruct((t, HEAD), BF16), jax.ShapeDtypeStruct((HEADS, t, HEAD), BF16)
    return [heads, tokens, tokens, heads, jax.ShapeDtypeStruct((HEADS, t), F32)]


def _all_shards(layer):
    return jax.ShapeDtypeStruct((DEVICES * PART, layer.shape[1]), BF16)


RING_SEMS = [pltpu.SemaphoreType.DMA((2 * CHIPS,))] * 4


def begin(first, layer, x):
    scratch = [pltpu.VMEM((DEVICES * PART, first.shape[1]), BF16), *ATTEND_SCRATCH] + [pltpu.SemaphoreType.DMA((CHIPS,))] * 4 + RING_SEMS
    shapes = _attention_shapes(x.shape[0]) + [_all_shards(layer)] + [jax.ShapeDtypeStruct((x.shape[0], HEAD), F32)] * 2
    return _remote_call(_begin, 1, shapes, scratch, (first, layer, x, *turns(x.shape[0])), "begin")


def _middle(layer_ref, o_ref, x_ref, near_ref, far_ref, w_ref, h1_ref, h2_ref, h3_ref, q_ref, k_ref, v_ref, o2_ref, lse_ref, all_ref,
            down_s, wo_s, top_s, mix_s, *sems):
    _, other, ring = _around()
    _meet([other, ring(1), ring(CHIPS - 1)])
    start, serve, finish = _ring(layer_ref, all_ref, *sems)
    start()
    _unfold_down(w_ref.at[:, pl.ds(2 * FF, FF)], down_s, DEVICES)
    _unfold_out(w_ref.at[:, pl.ds(FEED + QKV, QKV)], wo_s)
    tiles = x_ref.shape[0] // TILE

    def feed_tile(i, _):
        rows = pl.ds(pl.multiple_of(i * TILE, TILE), TILE)
        _feed_tile(rows, o_ref, x_ref, w_ref, h1_ref, h2_ref, down_s, wo_s)
        serve(i)

    lax.fori_loop(0, tiles, feed_tile, None)
    w = w_ref.at[:, pl.ds(FEED, QKV)]
    lax.fori_loop(0, tiles, lambda i, _: _project_rest(i, h2_ref, w, near_ref, far_ref, q_ref, k_ref, v_ref), None)
    serve(tiles)

    def attend_tile(i, _):
        _attend_tile(i, pl.ds(pl.multiple_of(i * TILE, TILE), TILE), q_ref, k_ref, v_ref, o2_ref, lse_ref, top_s, mix_s)
        pl.when((i == 1) | (i == 2))(lambda: serve(tiles + i, False))

    lax.fori_loop(0, tiles, attend_tile, None)
    finish()
    _unfold_out(all_ref.at[:, pl.ds(FEED, QKV)], wo_s)

    def join_tile(i, _):
        rows = pl.ds(pl.multiple_of(i * TILE, TILE), TILE)
        h3_ref[rows, :] = h2_ref[rows, :] + _mm(_heads(o2_ref, rows), wo_s[...]).astype(BF16)

    lax.fori_loop(0, tiles, join_tile, None)


def middle(layer, o, x, near, far, packed):
    t, d = x.shape
    scratch = [pltpu.VMEM((FF, d), BF16), pltpu.VMEM((ROW, d), BF16), *ATTEND_SCRATCH] + RING_SEMS
    shapes = [jax.ShapeDtypeStruct((t, d), BF16)] * 3 + _attention_shapes(t) + [_all_shards(layer)]
    return _remote_call(_middle, 5, shapes, scratch, (layer, o, x, near, far, packed), "middle")


def _scatter_phases(g_ref, o_ref, near_s, sent_s, far_s, pair_send, pair_recv, send, recv):
    me, chip, core = _place()
    other = me + 1 - 2 * core
    chips = [lax.rem(chip + k, CHIPS) * 2 for k in range(CHIPS)]
    pairs = [_send(g_ref.at[_rows(chips[k] + 1 - core), :], near_s.at[k], pair_send.at[k], pair_recv.at[k], other) for k in range(CHIPS)]
    copies = [_send(sent_s.at[k], far_s.at[k], send.at[k], recv.at[k], chips[k] + core) for k in range(1, CHIPS)]

    def both(k):
        return g_ref[_rows(chips[k] + core), :].astype(F32) + near_s[k].astype(F32)

    def starts():
        _meet([other] + [c + core for c in chips[1:]])
        for k in [*range(1, CHIPS), 0]:
            pairs[k].start()

    def passes():
        for k in range(1, CHIPS):
            pairs[k].wait_recv()
            sent_s[k] = both(k).astype(BF16)
            copies[k - 1].start()

    def ends():
        pairs[0].wait_recv()
        total = both(0)
        for k in range(1, CHIPS):
            copies[k - 1].wait_recv()
            total = total + far_s[k].astype(F32)
        o_ref[...] = total.astype(BF16)
        for copy in pairs + copies:
            copy.wait_send()

    return starts, passes, ends


def _scatter_scratch(g):
    return [pltpu.VMEM((CHIPS, PART, g.shape[1]), BF16)] * 3 + [pltpu.SemaphoreType.DMA((CHIPS,))] * 4


def _scatter(*refs):
    for phase in _scatter_phases(*refs):
        phase()


def scattered(g):
    return _remote_call(_scatter, 2, jax.ShapeDtypeStruct((PART, g.shape[1]), BF16), _scatter_scratch(g), (g,), "scattered")


def _squares(*refs):
    pieces, (o_ref, own_s, all_s, send, recv) = refs[:-5], refs[-5:]
    me, _, _ = _place()
    away = [lax.rem(me + k, DEVICES) for k in range(DEVICES)]

    def add_up():
        total = 0.0
        for ref in pieces:
            g = ref[...].astype(F32)
            total = total + jnp.sum(g * g)
        own_s[...] = jnp.full(own_s.shape, total, F32)

    _meet(away[1:], add_up)
    copies = [_send(own_s, all_s.at[me], send.at[k], recv.at[k], away[k]) for k in range(1, DEVICES)]
    for copy in copies:
        copy.start()
    all_s[me] = own_s[...]
    for copy in copies:
        copy.wait()
    o_ref[...] = all_s[...].sum(axis=0)


def squares(*pieces):
    tile, sems = (8, HEAD), pltpu.SemaphoreType.DMA((DEVICES,))
    return _remote_call(_squares, 3, jax.ShapeDtypeStruct(tile, F32), [pltpu.VMEM(tile, F32), pltpu.VMEM((DEVICES, *tile), F32), sems, sems], pieces, "squares")


def _pack(wq, wk, wv, wo, gate, up, down, first, layer0, layer1):
    def projections(out, at, n):
        for w in (wq, wk, wv):
            out[:, pl.ds(at, w.shape[2])] = w[n]
            at += w.shape[2]

    def rest(out, at, n):
        out[:, :FF] = gate[n]
        out[:, FF : 2 * FF] = up[n]
        for p in range(4):
            out[:, pl.ds(2 * FF + D * p, D)] = down[n, PART * p : PART * p + PART, :]
        for rows, columns, there, columns_there in _fold_map(0):
            out[there, pl.ds(at + columns_there.start, columns_there.size)] = wo[n, rows, columns]
        out[:, at + ROW :] = jnp.zeros((PART, STRIPE), BF16)

    projections(first, 0, 0)
    rest(layer0, FEED + QKV, 0)
    projections(layer0, FEED, 1)
    rest(layer1, FEED, 1)


def packed_weights(weights):
    shapes = [jax.ShapeDtypeStruct((PART, n), BF16) for n in (QKV, FEED + 2 * QKV, FEED + QKV)]
    return _call(_pack, (1,), [_whole(w.shape) for w in weights], [_whole(s.shape) for s in shapes], shapes, [], 10**6, weights, "pack")


def _adamw(*refs, count):
    (total_ref, *grads), refs = refs[:5], refs[5:]
    old, new = [refs[n : n + 7] for n in range(0, 21, 7)], [refs[n : n + 7] for n in range(21, 42, 7)]
    factor = jnp.minimum(1.0, 0.5 * lax.rsqrt(total_ref[:1, :1] / count + 1e-30))

    def update(name, layer, rows, columns, grad):
        i = NAMES.index(name)
        g = grad.astype(F32) * factor
        w, m, v = (one[i][layer, rows, columns] for one in old)
        w = w.astype(F32)
        m = 0.9 * m + 0.1 * g
        v = 0.95 * v + 0.05 * g * g
        step = m * lax.rsqrt(v + 1e-8) + 0.1 * w
        for one, value in zip(new, ((w - 0.02 * step).astype(BF16), m, v)):
            one[i][layer, rows, columns] = value

    every = slice(None)
    for layer in range(2):
        (feed, rest), at = grads[2 * layer : 2 * layer + 2], 0
        for name in ("wq", "wk", "wv"):
            width = old[0][NAMES.index(name)].shape[2]
            update(name, layer, every, every, rest[:, pl.ds(at, width)])
            at += width
        for rows, columns, there, columns_there in _fold_map(0):
            update("wo", layer, rows, columns, rest[there, pl.ds(at + columns_there.start, columns_there.size)])
        update("w_gate", layer, every, every, feed[:, :FF])
        update("w_up", layer, every, every, feed[:, FF : 2 * FF])
        for p in range(4):
            update("w_down", layer, pl.ds(PART * p, PART), every, feed[:, pl.ds(2 * FF + D * p, D)])


def adamw(total, grads, count, weights, m, v):
    args = (total, *grads, *weights, *m, *v)
    shapes = [jax.ShapeDtypeStruct(a.shape, a.dtype) for a in args[5:]]
    return _call(functools.partial(_adamw, count=count), (1,), [_whole(a.shape) for a in args], [_whole(s.shape) for s in shapes], shapes, [],
                 10**7, args, "adamw")


def solution(mesh):
    def scatter(gradient):
        return lax.psum_scatter(gradient, "dp", scatter_dimension=0, tiled=True)

    def step(x, dy, *arrays):
        weights, m, v = (arrays[i : i + 7] for i in (0, 7, 14))
        x, dy = x[0], dy[0]
        first, layer0, layer1 = packed_weights(weights)
        q0, k0, v0, o0, lse0, layer0, near, far = begin(first, layer0, x)
        mid0, h, mid1, q1, k1, v1, o1, lse1, layer1 = middle(layer1, o0, x, near, far, layer0)

        by_mid, feed1 = feed_back(mid1, dy, layer1)
        feed1 = scatter(feed1)
        by_o, delta, by_out = join_back(by_mid, o1, layer1, 6)
        dq, dk, dv = attended_back(q1, k1, v1, by_o, lse1, delta)
        by_h, rest1 = project_back(dq, dk, dv, near, far, h, by_out, by_mid, layer0, 6)

        by_mid, feed0 = feed_back(mid0, by_h, layer0)
        feed1, feed0 = lax.optimization_barrier((feed1, feed0))
        feed0 = scatter(feed0)
        by_o, delta, by_out = join_back(by_mid, o0, layer0, 7)
        dq, dk, dv, rest1 = attended_back(q0, k0, v0, by_o, lse0, delta, rest1)
        (rest0,) = project_back(dq, dk, dv, near, far, x, by_out)
        rest0 = scattered(rest0)

        grads = (feed0, rest0, feed1, rest1)
        total = squares(*grads)
        return tuple(adamw(total, grads, DEVICES * sum(g.size for g in grads), weights, m, v))

    states, cut = P(("rep", "dp"), None, None), P(None, "dp", None)
    return jax.shard_map(
        step,
        mesh=mesh,
        in_specs=(states, states) + (cut,) * 21,
        out_specs=(P("rep", "dp", None),) * 21,
        check_vma=False,
    )
```
